32 devices in a mesh: groups: 2 (over y), seq: 4 (over z), head: 2 (over x), rep: 2 (over core).
Axes of the slice: x: 2, y: 2, z: 4, core: 2. Of those that a mesh axis runs over, the one named last changes fastest.
Arguments:
- queries: bfloat16 [128, 64, 128], P(('groups', 'seq', 'rep'), 'head'), parts along dimension 0, may hold values from -256 to 256
- page_owner: int32 [128, 128], P(('groups', 'seq', 'rep')), parts along dimension 0, may hold values from -1 to 3, as said below
- page_slot: int32 [128, 128], P(('groups', 'seq', 'rep')), parts along dimension 0, may hold values from -1 to 63, as said below
- lengths: int32 [128], P(('groups', 'seq', 'rep')), parts along dimension 0, may hold values from 1 to 16384, as said below
- keys: bfloat16 [1024, 8, 128, 128], P(('groups', 'seq', 'rep'), 'head'), parts along dimension 0, may hold values from -24 to 24
- values: bfloat16 [1024, 8, 128, 128], P(('groups', 'seq', 'rep'), 'head'), parts along dimension 0, may hold values from -6 to 6
Outputs:
- attended: bfloat16 [128, 64, 128], P(('groups', 'seq', 'rep'), 'head'), parts along dimension 0
The draws below stay inside these ranges and needn't reach their ends.
There are 2 independent parts, one for each index of `groups`. The reference program is written for one: setup_inputs(seed, part) draws one part's arguments, and reference() takes and returns one part's arrays. A program takes and returns all parts, laid end to end along the dimension named above; each array names one. Nothing has to cross between parts.
Inputs may be any that keep to these rules, and one draw needn't show every extreme that they name: `page_owner`: for j below ceil(lengths[r] / 128) the seq index of the device, among those of r's half (r // 8) % 2, whose pool holds page j of r; -1 for later j. `page_slot`: the page's slot in that pool, -1 where page_owner is -1. No slot of a pool holds two pages; in each half, some device's pool has all 64 slots in use. `lengths`: in each half some request has the most.
All inputs are finite; a program needn't handle non-finite values.
Results may differ from the reference program's by a relative error of at most 0.0041.
Values may be sent and summed in bfloat16 or wider, within the bound.
A program may use at most 64 MiB of HBM per device.

```python
import math
import jax
import jax.numpy as jnp
from jax import lax

QH = 64
KVH = 8
HD = 128
PAGE = 128
MAXP = 128
REQ_DEV = 8
POOL_DEV = 64
REQ = 64
N_SEQ = 4
N_REP = 2


def page_layout(key):
    rows_half = REQ_DEV * N_SEQ
    total_pages = POOL_DEV * (N_SEQ + 1) // 2
    spare_pages = total_pages - rows_half
    extra_cells = rows_half * (MAXP - 1)
    slots_all = N_SEQ * POOL_DEV
    owner_list = []
    slot_list = []
    length_list = []
    for half_index in range(N_REP):
        half_keys = jax.random.split(jax.random.fold_in(key, 101 + half_index), 6)
        longest = jax.random.randint(half_keys[0], (), 0, rows_half)
        shuffled = jax.random.permutation(half_keys[1], extra_cells).astype(jnp.int32)
        cell_row = jnp.arange(extra_cells, dtype=jnp.int32) // (MAXP - 1)
        priority = jnp.where(cell_row == longest, shuffled - extra_cells, shuffled)
        ranked = jnp.argsort(priority)
        chosen = jnp.zeros((extra_cells,), jnp.int32).at[ranked[:spare_pages]].set(1)
        page_count = 1 + jnp.sum(chosen.reshape(rows_half, MAXP - 1), axis=1)
        tail_tokens = jax.random.randint(half_keys[2], (rows_half,), 1, PAGE + 1)
        tail_tokens = jnp.where(jnp.arange(rows_half) == longest, PAGE, tail_tokens)
        length_list.append((page_count - 1) * PAGE + tail_tokens)
        device_weight = jax.random.randint(half_keys[3], (N_SEQ,), 2, 5)
        lightest = jax.random.randint(half_keys[4], (), 0, N_SEQ)
        device_weight = jnp.where(jnp.arange(N_SEQ) == lightest, 1, device_weight)
        tie_break = jax.random.permutation(half_keys[5], slots_all).astype(jnp.int32)
        slot_ids = jnp.arange(slots_all, dtype=jnp.int32)
        slot_score = slot_ids % POOL_DEV * device_weight[slot_ids // POOL_DEV] * slots_all + tie_break
        picked = jnp.argsort(slot_score)[:total_pages].astype(jnp.int32)
        first_page = jnp.cumsum(page_count) - page_count
        page_index = jnp.arange(MAXP, dtype=jnp.int32)
        page_used = page_index[None, :] < page_count[:, None]
        flat_index = jnp.clip(first_page[:, None] + page_index[None, :], 0, total_pages - 1)
        chosen_slot = picked[flat_index]
        owner_list.append(jnp.where(page_used, chosen_slot // POOL_DEV, -1))
        slot_list.append(jnp.where(page_used, chosen_slot % POOL_DEV, -1))

    def arrange(pieces):
        tail_shape = pieces[0].shape[1:]
        stacked = jnp.stack(pieces).reshape((N_REP, N_SEQ, REQ_DEV) + tail_shape)
        stacked = jnp.moveaxis(stacked, 0, 1)
        return stacked.reshape((REQ,) + tail_shape).astype(jnp.int32)
    return (arrange(owner_list), arrange(slot_list), arrange(length_list))


def draw_page_owner(key, part):
    return page_layout(key)[0]


def draw_page_slot(key, part):
    return page_layout(key)[1]


def draw_lengths(key, part):
    return page_layout(key)[2]


def draw_keys(key, part):
    full_shape = (N_SEQ * N_REP * POOL_DEV, KVH, PAGE, HD)
    sample = jax.random.normal(jax.random.fold_in(key, 11), full_shape, jnp.float32)
    return jnp.clip(sample, -24.0, 24.0).astype(jnp.bfloat16)


def draw_queries(key, part):
    full_shape = (REQ, QH, HD)
    sample = jax.random.normal(jax.random.fold_in(key, 23), full_shape, jnp.float32)
    return jnp.clip(sample, -256.0, 256.0).astype(jnp.bfloat16)


def levels(rng, dims, cuts, least, top_value):
    gain = 1.0
    for dim, shards_of in cuts:
        heights = jax.random.uniform(jax.random.fold_in(jax.random.fold_in(rng, 6), dim), (shards_of,), jnp.float32, least / len(cuts), top_value / len(cuts))
        gain = gain * jnp.repeat(jnp.exp(heights), dims[dim] // shards_of).reshape((-1,) + (1,) * (len(dims) - 1 - dim))
    return gain


def bell_draw(stream_key, dims, scale, bound, cuts=(), kind=jnp.bfloat16):
    result = jax.random.normal(stream_key, dims, jnp.float32) * scale
    if len(cuts) > 0:
        result = levels(stream_key, dims, cuts, -0.22, 0.18) * result
    return jnp.clip(result, min=-bound, max=bound).astype(kind)


def setup_inputs(seed: int = 0, part: int = 0) -> dict:
    key_of = jax.random.split(jax.random.key(seed), 7)
    part_splits = jax.random.split(jax.random.fold_in(key_of[6], part), 7)
    queries = draw_queries(jax.random.fold_in(jax.random.fold_in(key_of[6], part), 71), part)
    page_owner = draw_page_owner(jax.random.fold_in(jax.random.fold_in(key_of[6], part), 71), part)
    page_slot = draw_page_slot(jax.random.fold_in(jax.random.fold_in(key_of[6], part), 71), part)
    lengths = draw_lengths(jax.random.fold_in(jax.random.fold_in(key_of[6], part), 71), part)
    keys = draw_keys(jax.random.fold_in(jax.random.fold_in(key_of[6], part), 71), part)
    values = bell_draw(part_splits[5], (N_SEQ * N_REP * POOL_DEV, KVH, PAGE, HD), 1.0, 6.0, ((0, 8), (1, 2)))
    return {"queries": queries, "page_owner": page_owner, "page_slot": page_slot, "lengths": lengths, "keys": keys, "values": values}


masked_score = -1e+30

def reference(queries, page_owner, page_slot, lengths, keys, values):
    request_count = queries.shape[0]
    group_size = QH // KVH
    score_scale = 1.0 / math.sqrt(HD)
    half_index = (jnp.arange(request_count, dtype=jnp.int32) // REQ_DEV % N_REP).astype(jnp.int32)
    page_index = jnp.arange(MAXP, dtype=jnp.int32)
    token_index = jnp.arange(PAGE, dtype=jnp.int32)

    def attend_one(request_data):
        single_query, owner_row, slot_row, token_count, half_side = request_data
        pool_index = ((jnp.maximum(owner_row, 0) * N_REP + half_side) * POOL_DEV + jnp.maximum(slot_row, 0)).astype(jnp.int32)
        page_keys = keys[pool_index].astype(jnp.float32)
        page_values = values[pool_index].astype(jnp.float32)
        grouped_query = single_query.astype(jnp.float32).reshape(KVH, group_size, HD)
        scores = jnp.einsum('kgd,jktd->jkgt', grouped_query, page_keys, precision=lax.Precision.HIGHEST) * score_scale
        live_count = jnp.clip(token_count - page_index * PAGE, 0, PAGE)
        live_tokens = (token_index[None, :] < live_count[:, None])[:, None, None, :]
        scores = jnp.where(live_tokens, scores, masked_score)
        page_max = lax.optimization_barrier(jnp.max(scores, axis=3))
        weights = jnp.where(live_tokens, jnp.exp(scores - page_max[..., None]), 0.0)
        page_sum = lax.optimization_barrier(jnp.sum(weights, axis=3))
        rounded = lax.optimization_barrier(weights.astype(jnp.bfloat16))
        page_out = jnp.einsum('jkgt,jktd->jkgd', rounded.astype(jnp.float32), page_values, precision=lax.Precision.HIGHEST)
        live_pages = (live_count > 0)[:, None, None]
        request_top = lax.optimization_barrier(jnp.max(jnp.where(live_pages, page_max, masked_score), axis=0))
        rescale = jnp.where(live_pages, jnp.exp(jnp.minimum(page_max - request_top[None], 0.0)), 0.0)
        request_total = lax.optimization_barrier(jnp.sum(rescale * page_sum, axis=0))
        request_out = lax.optimization_barrier(jnp.sum(rescale[..., None] * page_out, axis=0))
        return (request_out / request_total[..., None]).astype(jnp.bfloat16).reshape(QH, HD)
    return lax.map(attend_one, (queries, page_owner, page_slot, lengths, half_index))
```

```python
import functools
import math

import jax
import jax.numpy as jnp
from jax import lax
from jax.experimental import pallas as pl
from jax.experimental.pallas import tpu as pltpu
from jax.sharding import PartitionSpec as P

MASKED = -1e30
F32 = jnp.float32
BF16 = jnp.bfloat16
NT = (((1,), (1,)), ((), ()))


def iota(shape, dim):
    return lax.broadcasted_iota(jnp.int32, shape, dim)


def kernel(
    n, lens_ref, q_ref, owner_ref, slot_ref, k_hbm, v_hbm, out_ref,
    kbuf, vbuf, qall, tsend, trecv, liveb, reqb, mt, m, qslot, wbuf, ohi,
    osend, orecv, ssend, srecv,
    ksem, vsem, tss, trs, qss, qrs, oss, ors, sss, srs,
):
    pool, kv, tokens, width = k_hbm.shape
    rows = q_ref.shape[0]
    group = q_ref.shape[1] // kv
    block = rows * group
    lanes = trecv.shape[2]
    scale = math.log2(math.e) / math.sqrt(width)
    me = lax.axis_index("seq")

    def peer(off):
        return {"seq": lax.rem(me + off, n)}

    def source(off):
        return {"seq": lax.rem(me + n - off, n)}

    def remote(src, dst, ssem, rsem, to):
        return pltpu.make_async_remote_copy(
            src_ref=src, dst_ref=dst, send_sem=ssem, recv_sem=rsem,
            device_id=to, device_id_type=pl.DeviceIdType.MESH,
        )

    barrier = pltpu.get_barrier_semaphore()
    for off in range(1, n):
        pl.semaphore_signal(
            barrier, inc=1, device_id=peer(off), device_id_type=pl.DeviceIdType.MESH
        )
    kcopies = [pltpu.make_async_copy(k_hbm.at[:, h], kbuf.at[h], ksem.at[h]) for h in range(kv)]
    vcopies = [pltpu.make_async_copy(v_hbm.at[:, h], vbuf.at[h], vsem.at[h]) for h in range(kv)]
    for h in range(kv):
        kcopies[h].start()
        vcopies[h].start()

    queries = q_ref[...].astype(F32).reshape(rows, kv, group, width)
    for h in range(kv):
        qall[h, 0:block, :] = queries[:, h].reshape(block, width).astype(BF16)

    span = owner_ref.shape[1]
    row = iota((rows, span), 0)
    length = jnp.zeros((rows, span), jnp.int32)
    for r in range(rows):
        length = jnp.where(row == r, lens_ref[r], length)
    live = jnp.clip(length - iota((rows, span), 1) * tokens, 0, tokens)
    live_f = live.astype(F32)
    owner = owner_ref[...]
    slot = slot_ref[...]
    ones = jnp.ones((8, span), BF16)
    slot_id = iota((pool, span), 0)
    for off in range(n):
        there = lax.rem(me + off, n)
        key = jnp.where((owner == there) & (live > 0), slot, -1)
        acc_live = jnp.zeros((pool, span), F32)
        acc_req = jnp.zeros((pool, span), F32)
        for r in range(rows):
            hit = slot_id == key[r : r + 1, :]
            acc_live = jnp.where(hit, live_f[r : r + 1, :], acc_live)
            acc_req = jnp.where(hit, float(r + 1), acc_req)
        t_live = lax.dot_general(ones, acc_live.astype(BF16), NT, preferred_element_type=F32)
        t_req = lax.dot_general(ones, acc_req.astype(BF16), NT, preferred_element_type=F32)
        table = jnp.where(iota((8, pool), 0) == 0, t_live, t_req)
        if lanes > pool:
            table = jnp.concatenate([table, jnp.zeros((8, lanes - pool), F32)], axis=1)
        if off == 0:
            trecv[0] = table
        else:
            tsend[off] = table

    pl.semaphore_wait(barrier, n - 1)
    tcopies = {}
    qcopies = {}
    for off in range(1, n):
        tcopies[off] = remote(
            tsend.at[off], trecv.at[off], tss.at[off], trs.at[off], peer(off)
        )
        tcopies[off].start()
    for h in range(kv):
        for off in range(1, n):
            qcopies[h, off] = remote(
                qall.at[h, pl.ds(0, block)],
                qall.at[h, pl.ds(off * block, block)],
                qss.at[h, off], qrs.at[h, off], peer(off),
            )
            qcopies[h, off].start()

    for off in range(1, n):
        tcopies[off].wait_recv()
    live_row = trecv[0][0:1, :]
    req_row = trecv[0][1:2, :]
    for off in range(1, n):
        t = trecv[off]
        live_row = live_row + t[0:1, :]
        req_row = req_row + jnp.where(t[1:2, :] > 0.0, t[1:2, :] + float(off * rows), 0.0)
    pg = pool * group
    spread = jnp.where(iota((pg, lanes), 0) // group == iota((pg, lanes), 1), 1.0, 0.0)
    spread = spread.astype(BF16)
    liveb[...] = lax.dot_general(
        spread, jnp.broadcast_to(live_row, (128, lanes)).astype(BF16), NT,
        preferred_element_type=F32,
    )
    reqb[...] = lax.dot_general(
        spread, jnp.broadcast_to(req_row, (128, lanes)).astype(BF16), NT,
        preferred_element_type=F32,
    )
    same = iota((pg, 128), 0) % group == iota((pg, 128), 1) % group
    for c in range(n * block // 128):
        want = ((iota((pg, 128), 1) + c * 128) // group + 1).astype(F32)
        mt[:, c * 128 : (c + 1) * 128] = jnp.where(
            same & (reqb[...] == want), 1.0, 0.0
        ).astype(BF16)
    spread_t = jnp.where(iota((lanes, pg), 0) == iota((lanes, pg), 1) // group, 1.0, 0.0)
    req_wide = jnp.dot(
        jnp.broadcast_to(req_row, (8, lanes)).astype(BF16), spread_t.astype(BF16),
        preferred_element_type=F32,
    )[0:1, :]
    same_t = iota((block, pg), 0) % group == iota((block, pg), 1) % group
    for off in range(n):
        want = (iota((block, pg), 0) // group + (off * rows + 1)).astype(F32)
        m[off * block : (off + 1) * block, :] = jnp.where(
            same_t & (req_wide == want), 1.0, 0.0
        ).astype(BF16)

    lane_f = iota((group, 128), 1).astype(F32)
    lane = iota((group, 128), 1)
    pair = 2 * group
    tops = []
    sums = []
    ocopies = {}
    scopies = {}
    for h in range(kv):
        for off in range(1, n):
            qcopies[h, off].wait_recv()
        qslot[...] = jnp.dot(mt[...], qall[h], preferred_element_type=F32).astype(BF16)
        kcopies[h].wait()

        top = jnp.full((group, 128), MASKED, F32)
        for i in range(pool // 2):
            keys = kbuf[h, 2 * i : 2 * i + 2].reshape(2 * tokens, width)
            s = lax.dot_general(
                qslot[i * pair : (i + 1) * pair, :], keys, NT, preferred_element_type=F32
            )
            for u in range(2):
                at = slice((2 * i + u) * group, (2 * i + u + 1) * group)
                x = s[u * group : (u + 1) * group, u * tokens : (u + 1) * tokens]
                x = jnp.where(lane_f < liveb[at, :], x * scale, MASKED)
                wbuf[at, :] = x
                pm = jnp.max(x, axis=1, keepdims=True)
                top = jnp.maximum(top, jnp.where(reqb[at, :] == lane_f + 1.0, pm, MASKED))
        vcopies[h].wait()

        acc = jnp.zeros((group, 128), F32)
        for i in range(pool // 2):
            weights = []
            for u in range(2):
                at = slice((2 * i + u) * group, (2 * i + u + 1) * group)
                mine = reqb[at, :] == lane_f + 1.0
                rm = jnp.max(jnp.where(mine, top, MASKED), axis=1, keepdims=True)
                w = jnp.exp2(wbuf[at, :] - rm)
                acc = acc + jnp.where(mine, jnp.sum(w, axis=1, keepdims=True), 0.0)
                weights.append(w)
            both = jnp.concatenate([vbuf[h, 2 * i], vbuf[h, 2 * i + 1]], axis=1)
            out = jnp.dot(
                jnp.concatenate(weights, axis=0).astype(BF16), both, preferred_element_type=F32
            )
            ohi[i * pair : (i + 1) * pair, :] = jnp.concatenate(
                [out[u * group : (u + 1) * group, u * width : (u + 1) * width] for u in range(2)],
                axis=0,
            ).astype(BF16)
        tops.append(top)
        sums.append(acc)
        if h == kv - 1:
            for off in range(n):
                stat = jnp.zeros((group, 128), F32)
                for g in range(kv):
                    for j, x in enumerate((tops[g], sums[g])):
                        at = (2 * g + j) * rows
                        shift = (at - off * rows) % 128
                        y = pltpu.roll(x, shift, 1) if shift else x
                        stat = jnp.where((lane >= at) & (lane < at + rows), y, stat)
                if off == 0:
                    srecv[0] = stat
                else:
                    ssend[off] = stat
                    scopies[off] = remote(
                        ssend.at[off], srecv.at[off], sss.at[off], srs.at[off], source(off)
                    )
                    scopies[off].start()
        osend[h] = jnp.dot(m[...], ohi[...], preferred_element_type=F32).astype(BF16)
        for off in range(1, n):
            ocopies[h, off] = remote(
                osend.at[h, pl.ds(off * block, block)], orecv.at[h, off],
                oss.at[h, off], ors.at[h, off], source(off),
            )
            ocopies[h, off].start()

    for off in range(1, n):
        scopies[off].wait_recv()
    stats = [srecv[off] for off in range(n)]
    best = functools.reduce(jnp.maximum, stats)
    factors = [jnp.exp2(x - best) for x in stats]
    whole = functools.reduce(
        jnp.add, [f * pltpu.roll(x, 128 - rows, 1) for f, x in zip(factors, stats)]
    )
    factors = [f / whole for f in factors]
    parts = []
    for h in range(kv):
        gathered = []
        for off in range(n):
            if off == 0:
                got = osend[h, 0:block, :]
            else:
                ocopies[h, off].wait_recv()
                got = orecv[h, off]
            gathered.append(got.astype(F32).reshape(rows, group, width))
        per_row = []
        for r in range(rows):
            at = 2 * h * rows + r
            total = factors[0][:, at : at + 1] * gathered[0][r]
            for off in range(1, n):
                total = total + factors[off][:, at : at + 1] * gathered[off][r]
            per_row.append(total)
        parts.append(per_row)
    for r in range(rows):
        out_ref[r] = jnp.concatenate([parts[h][r] for h in range(kv)], axis=0).astype(BF16)

    for off in range(1, n):
        tcopies[off].wait_send()
        scopies[off].wait_send()
        for h in range(kv):
            qcopies[h, off].wait_send()
            ocopies[h, off].wait_send()


def on_device(n, queries, page_owner, page_slot, lengths, keys, values):
    pool, kv, tokens, width = keys.shape
    rows, heads, _ = queries.shape
    group = heads // kv
    block = rows * group
    pg = pool * group
    lanes = -(-pool // 128) * 128
    dma = pltpu.SemaphoreType.DMA
    vmem = pl.BlockSpec(memory_space=pltpu.VMEM)
    return pl.pallas_call(
        functools.partial(kernel, n),
        out_shape=jax.ShapeDtypeStruct(queries.shape, BF16),
        in_specs=[
            pl.BlockSpec(memory_space=pltpu.SMEM),
            vmem,
            vmem,
            vmem,
            pl.BlockSpec(memory_space=pl.ANY),
            pl.BlockSpec(memory_space=pl.ANY),
        ],
        out_specs=vmem,
        scratch_shapes=[
            pltpu.VMEM((kv, pool, tokens, width), BF16),
            pltpu.VMEM((kv, pool, tokens, width), BF16),
            pltpu.VMEM((kv, n * block, width), BF16),
            pltpu.VMEM((n, 8, lanes), F32),
            pltpu.VMEM((n, 8, lanes), F32),
            pltpu.VMEM((pg, 128), F32),
            pltpu.VMEM((pg, 128), F32),
            pltpu.VMEM((pg, n * block), BF16),
            pltpu.VMEM((n * block, pg), BF16),
            pltpu.VMEM((pg, width), BF16),
            pltpu.VMEM((pg, tokens), F32),
            pltpu.VMEM((pg, width), BF16),
            pltpu.VMEM((kv, n * block, width), BF16),
            pltpu.VMEM((kv, n, block, width), BF16),
            pltpu.VMEM((n, group, 128), F32),
            pltpu.VMEM((n, group, 128), F32),
            dma((kv,)), dma((kv,)),
            dma((n,)), dma((n,)),
            dma((kv, n)), dma((kv, n)),
            dma((kv, n)), dma((kv, n)),
            dma((n,)), dma((n,)),
        ],
        compiler_params=pltpu.CompilerParams(
            collective_id=0, has_side_effects=True, vmem_limit_bytes=60 * 1024 * 1024
        ),
        name="paged",
    )(lengths, queries, page_owner, page_slot, keys, values)


def solution(mesh):
    placed = (
        P(("groups", "seq", "rep"), "head", None),
        P(("groups", "seq", "rep"), None),
        P(("groups", "seq", "rep"), None),
        P(("groups", "seq", "rep")),
        P(("groups", "seq", "rep"), "head", None, None),
        P(("groups", "seq", "rep"), "head", None, None),
    )
    return jax.shard_map(
        functools.partial(on_device, mesh.shape["seq"]),
        mesh=mesh,
        in_specs=placed,
        out_specs=P(("groups", "seq", "rep"), "head", None),
        check_vma=False,
    )
```

```python
import functools
import math

import jax
import jax.numpy as jnp
from jax import lax
from jax.experimental import pallas as pl
from jax.experimental.pallas import tpu as pltpu
from jax.sharding import PartitionSpec as P

MASKED = -1e30
F32 = jnp.float32
BF16 = jnp.bfloat16
NT = (((1,), (1,)), ((), ()))


def iota(shape, dim):
    return lax.broadcasted_iota(jnp.int32, shape, dim)


def kernel(
    n, lens_hbm, q_hbm, owner_hbm, slot_hbm, k_hbm, v_hbm, out_ref,
    lens_ref, q_ref, owner_ref, slot_ref, kbuf, vbuf, qall, tsend, trecv, liveb, reqb, mt, m, qslot, wbuf, ohi,
    osend, orecv, ssend, srecv,
    isem, ksem, vsem, tss, trs, qss, qrs, oss, ors, sss, srs,
):
    pool, kv, tokens, width = k_hbm.shape
    rows = q_hbm.shape[0]
    group = q_hbm.shape[1] // kv
    block = rows * group
    lanes = trecv.shape[2]
    scale = math.log2(math.e) / math.sqrt(width)
    me = lax.axis_index("seq")

    def peer(off):
        return {"seq": lax.rem(me + off, n)}

    def source(off):
        return {"seq": lax.rem(me + n - off, n)}

    def remote(src, dst, ssem, rsem, to):
        return pltpu.make_async_remote_copy(
            src_ref=src, dst_ref=dst, send_sem=ssem, recv_sem=rsem,
            device_id=to, device_id_type=pl.DeviceIdType.MESH,
        )

    barrier = pltpu.get_barrier_semaphore()
    for off in range(1, n):
        pl.semaphore_signal(
            barrier, inc=1, device_id=peer(off), device_id_type=pl.DeviceIdType.MESH
        )
    icopies = [
        pltpu.make_async_copy(src, dst, isem.at[i])
        for i, (src, dst) in enumerate((
            (lens_hbm, lens_ref), (owner_hbm, owner_ref), (slot_hbm, slot_ref), (q_hbm, q_ref),
        ))
    ]
    for copy in icopies:
        copy.start()
    kcopies = [pltpu.make_async_copy(k_hbm.at[:, h], kbuf.at[h], ksem.at[h]) for h in range(kv)]
    vcopies = [pltpu.make_async_copy(v_hbm.at[:, h], vbuf.at[h], vsem.at[h]) for h in range(kv)]

    for copy in icopies:
        copy.wait()
    for h in range(kv):
        kcopies[h].start()
        vcopies[h].start()
    span = owner_ref.shape[1]
    row = iota((rows, span), 0)
    length = jnp.zeros((rows, span), jnp.int32)
    for r in range(rows):
        length = jnp.where(row == r, lens_ref[r], length)
    live = jnp.clip(length - iota((rows, span), 1) * tokens, 0, tokens)
    live_f = live.astype(F32)
    owner = owner_ref[...]
    slot = slot_ref[...]
    ones = jnp.ones((8, span), BF16)
    slot_id = iota((pool, span), 0)
    for off in range(n):
        there = lax.rem(me + off, n)
        key = jnp.where((owner == there) & (live > 0), slot, -1)
        acc_live = jnp.zeros((pool, span), F32)
        acc_req = jnp.zeros((pool, span), F32)
        for r in range(rows):
            hit = slot_id == key[r : r + 1, :]
            acc_live = jnp.where(hit, live_f[r : r + 1, :], acc_live)
            acc_req = jnp.where(hit, float(r + 1), acc_req)
        t_live = lax.dot_general(ones, acc_live.astype(BF16), NT, preferred_element_type=F32)
        t_req = lax.dot_general(ones, acc_req.astype(BF16), NT, preferred_element_type=F32)
        table = jnp.where(iota((8, pool), 0) == 0, t_live, t_req)
        if lanes > pool:
            table = jnp.concatenate([table, jnp.zeros((8, lanes - pool), F32)], axis=1)
        if off == 0:
            trecv[0] = table
        else:
            tsend[off] = table

    queries = q_ref[...].astype(F32).reshape(rows, kv, group, width)
    for h in range(kv):
        qall[h, 0:block, :] = queries[:, h].reshape(block, width).astype(BF16)

    pl.semaphore_wait(barrier, n - 1)
    tcopies = {}
    qcopies = {}
    for off in range(1, n):
        tcopies[off] = remote(
            tsend.at[off], trecv.at[off], tss.at[off], trs.at[off], peer(off)
        )
        tcopies[off].start()
    for h in range(kv):
        for off in range(1, n):
            qcopies[h, off] = remote(
                qall.at[h, pl.ds(0, block)],
                qall.at[h, pl.ds(off * block, block)],
                qss.at[h, off], qrs.at[h, off], peer(off),
            )

    def send(first, last):
        for h in range(first, last):
            for off in range(1, n):
                qcopies[h, off].start()

    early = lax.axis_index("rep") == 0

    @pl.when(early)
    def _():
        send(0, kv)

    for off in range(1, n):
        tcopies[off].wait_recv()

    @pl.when(jnp.logical_not(early))
    def _():
        send(0, kv)

    live_row = trecv[0][0:1, :]
    req_row = trecv[0][1:2, :]
    for off in range(1, n):
        t = trecv[off]
        live_row = live_row + t[0:1, :]
        req_row = req_row + jnp.where(t[1:2, :] > 0.0, t[1:2, :] + float(off * rows), 0.0)
    pg = pool * group
    spread = jnp.where(iota((pg, lanes), 0) // group == iota((pg, lanes), 1), 1.0, 0.0)
    spread = spread.astype(BF16)
    liveb[...] = lax.dot_general(
        spread, jnp.broadcast_to(live_row, (128, lanes)).astype(BF16), NT,
        preferred_element_type=F32,
    )
    reqb[...] = lax.dot_general(
        spread, jnp.broadcast_to(req_row, (128, lanes)).astype(BF16), NT,
        preferred_element_type=F32,
    )
    same = iota((pg, 128), 0) % group == iota((pg, 128), 1) % group
    for c in range(n * block // 128):
        want = ((iota((pg, 128), 1) + c * 128) // group + 1).astype(F32)
        mt[:, c * 128 : (c + 1) * 128] = jnp.where(
            same & (reqb[...] == want), 1.0, 0.0
        ).astype(BF16)
    spread_t = jnp.where(iota((lanes, pg), 0) == iota((lanes, pg), 1) // group, 1.0, 0.0)
    req_wide = jnp.dot(
        jnp.broadcast_to(req_row, (8, lanes)).astype(BF16), spread_t.astype(BF16),
        preferred_element_type=F32,
    )[0:1, :]
    same_t = iota((block, pg), 0) % group == iota((block, pg), 1) % group
    for off in range(n):
        want = (iota((block, pg), 0) // group + (off * rows + 1)).astype(F32)
        m[off * block : (off + 1) * block, :] = jnp.where(
            same_t & (req_wide == want), 1.0, 0.0
        ).astype(BF16)

    lane_f = iota((group, 128), 1).astype(F32)
    lane = iota((group, 128), 1)
    pair = 2 * group
    tops = []
    sums = []
    ocopies = {}
    scopies = {}
    for h in range(kv):
        for off in range(1, n):
            qcopies[h, off].wait_recv()
        qslot[...] = jnp.dot(mt[...], qall[h], preferred_element_type=F32).astype(BF16)
        kcopies[h].wait()

        top = jnp.full((group, 128), MASKED, F32)
        for i in range(pool // 2):
            keys = kbuf[h, 2 * i : 2 * i + 2].reshape(2 * tokens, width)
            s = lax.dot_general(
                qslot[i * pair : (i + 1) * pair, :], keys, NT, preferred_element_type=F32
            )
            for u in range(2):
                at = slice((2 * i + u) * group, (2 * i + u + 1) * group)
                x = s[u * group : (u + 1) * group, u * tokens : (u + 1) * tokens]
                x = jnp.where(lane_f < liveb[at, :], x * scale, MASKED)
                wbuf[at, :] = x
                pm = jnp.max(x, axis=1, keepdims=True)
                top = jnp.maximum(top, jnp.where(reqb[at, :] == lane_f + 1.0, pm, MASKED))
        vcopies[h].wait()

        acc = jnp.zeros((group, 128), F32)
        for i in range(pool // 2):
            weights = []
            for u in range(2):
                at = slice((2 * i + u) * group, (2 * i + u + 1) * group)
                mine = reqb[at, :] == lane_f + 1.0
                rm = jnp.max(jnp.where(mine, top, MASKED), axis=1, keepdims=True)
                w = jnp.exp2(wbuf[at, :] - rm)
                acc = acc + jnp.where(mine, jnp.sum(w, axis=1, keepdims=True), 0.0)
                weights.append(w)
            both = jnp.concatenate([vbuf[h, 2 * i], vbuf[h, 2 * i + 1]], axis=1)
            out = jnp.dot(
                jnp.concatenate(weights, axis=0).astype(BF16), both, preferred_element_type=F32
            )
            ohi[i * pair : (i + 1) * pair, :] = jnp.concatenate(
                [out[u * group : (u + 1) * group, u * width : (u + 1) * width] for u in range(2)],
                axis=0,
            ).astype(BF16)
        tops.append(top)
        sums.append(acc)
        if h == kv - 1:
            for off in range(n):
                stat = jnp.zeros((group, 128), F32)
                for g in range(kv):
                    for j, x in enumerate((tops[g], sums[g])):
                        at = (2 * g + j) * rows
                        shift = (at - off * rows) % 128
                        y = pltpu.roll(x, shift, 1) if shift else x
                        stat = jnp.where((lane >= at) & (lane < at + rows), y, stat)
                if off == 0:
                    srecv[0] = stat
                else:
                    ssend[off] = stat
                    scopies[off] = remote(
                        ssend.at[off], srecv.at[off], sss.at[off], srs.at[off], source(off)
                    )
                    scopies[off].start()
        osend[h] = jnp.dot(m[...], ohi[...], preferred_element_type=F32).astype(BF16)
        for off in range(1, n):
            ocopies[h, off] = remote(
                osend.at[h, pl.ds(off * block, block)], orecv.at[h, off],
                oss.at[h, off], ors.at[h, off], source(off),
            )
            ocopies[h, off].start()

    for off in range(1, n):
        scopies[off].wait_recv()
    stats = [srecv[off] for off in range(n)]
    best = functools.reduce(jnp.maximum, stats)
    factors = [jnp.exp2(x - best) for x in stats]
    whole = functools.reduce(
        jnp.add, [f * pltpu.roll(x, 128 - rows, 1) for f, x in zip(factors, stats)]
    )
    factors = [f / whole for f in factors]
    parts = []
    for h in range(kv):
        gathered = []
        for off in range(n):
            if off == 0:
                got = osend[h, 0:block, :]
            else:
                ocopies[h, off].wait_recv()
                got = orecv[h, off]
            gathered.append(got.astype(F32).reshape(rows, group, width))
        per_row = []
        for r in range(rows):
            at = 2 * h * rows + r
            total = factors[0][:, at : at + 1] * gathered[0][r]
            for off in range(1, n):
                total = total + factors[off][:, at : at + 1] * gathered[off][r]
            per_row.append(total)
        parts.append(per_row)
    for r in range(rows):
        out_ref[r] = jnp.concatenate([parts[h][r] for h in range(kv)], axis=0).astype(BF16)

    for off in range(1, n):
        tcopies[off].wait_send()
        scopies[off].wait_send()
        for h in range(kv):
            qcopies[h, off].wait_send()
            ocopies[h, off].wait_send()


def on_device(n, queries, page_owner, page_slot, lengths, keys, values):
    pool, kv, tokens, width = keys.shape
    rows, heads, _ = queries.shape
    group = heads // kv
    block = rows * group
    pg = pool * group
    lanes = -(-pool // 128) * 128
    dma = pltpu.SemaphoreType.DMA
    vmem = pl.BlockSpec(memory_space=pltpu.VMEM)
    return pl.pallas_call(
        functools.partial(kernel, n),
        out_shape=pltpu.VMEM(queries.shape, BF16),
        in_specs=[pl.BlockSpec(memory_space=pl.ANY)] * 6,
        out_specs=vmem,
        scratch_shapes=[
            pltpu.SMEM(lengths.shape, jnp.int32),
            pltpu.VMEM(queries.shape, BF16),
            pltpu.VMEM(page_owner.shape, jnp.int32),
            pltpu.VMEM(page_slot.shape, jnp.int32),
            pltpu.VMEM((kv, pool, tokens, width), BF16),
            pltpu.VMEM((kv, pool, tokens, width), BF16),
            pltpu.VMEM((kv, n * block, width), BF16),
            pltpu.VMEM((n, 8, lanes), F32),
            pltpu.VMEM((n, 8, lanes), F32),
            pltpu.VMEM((pg, 128), F32),
            pltpu.VMEM((pg, 128), F32),
            pltpu.VMEM((pg, n * block), BF16),
            pltpu.VMEM((n * block, pg), BF16),
            pltpu.VMEM((pg, width), BF16),
            pltpu.VMEM((pg, tokens), F32),
            pltpu.VMEM((pg, width), BF16),
            pltpu.VMEM((kv, n * block, width), BF16),
            pltpu.VMEM((kv, n, block, width), BF16),
            pltpu.VMEM((n, group, 128), F32),
            pltpu.VMEM((n, group, 128), F32),
            dma((4,)), dma((kv,)), dma((kv,)),
            dma((n,)), dma((n,)),
            dma((kv, n)), dma((kv, n)),
            dma((kv, n)), dma((kv, n)),
            dma((n,)), dma((n,)),
        ],
        compiler_params=pltpu.CompilerParams(
            collective_id=0, has_side_effects=True, vmem_limit_bytes=66977792
        ),
        name="paged",
    )(lengths, queries, page_owner, page_slot, keys, values)


def solution(mesh):
    placed = (
        P(("groups", "seq", "rep"), "head", None),
        P(("groups", "seq", "rep"), None),
        P(("groups", "seq", "rep"), None),
        P(("groups", "seq", "rep")),
        P(("groups", "seq", "rep"), "head", None, None),
        P(("groups", "seq", "rep"), "head", None, None),
    )
    return jax.shard_map(
        functools.partial(on_device, mesh.shape["seq"]),
        mesh=mesh,
        in_specs=placed,
        out_specs=P(("groups", "seq", "rep"), "head", None),
        check_vma=False,
    )
```

```python
import functools
import math

import jax
import jax.numpy as jnp
from jax import lax
from jax.experimental import pallas as pl
from jax.experimental.pallas import tpu as pltpu
from jax.sharding import PartitionSpec as P

MASKED = -1e30
CODE = 256.0
LATE = 0
DEPTH = 3
F32 = jnp.float32
BF16 = jnp.bfloat16
NT = (((1,), (1,)), ((), ()))


def iota(shape, dim):
    return lax.broadcasted_iota(jnp.int32, shape, dim)


def kernel(
    n, lens_hbm, q_hbm, owner_hbm, slot_hbm, k_hbm, v_hbm, out_ref,
    lens_ref, q_ref, owner_ref, slot_ref, kbuf, vbuf, qall, tsend, trecv, liveb, reqb, mt, m, qslot, wbuf, ohi,
    osend, orecv, ssend, srecv,
    isem, ksem, vsem, tss, trs, qss, qrs, oss, ors, sss, srs,
):
    pool, kv, tokens, width = k_hbm.shape
    rows = q_hbm.shape[0]
    group = q_hbm.shape[1] // kv
    block = rows * group
    lanes = trecv.shape[2]
    scale = math.log2(math.e) / math.sqrt(width)
    me = lax.axis_index("seq")

    def peer(off):
        return {"seq": lax.rem(me + off, n)}

    def source(off):
        return {"seq": lax.rem(me + n - off, n)}

    def remote(src, dst, ssem, rsem, to):
        return pltpu.make_async_remote_copy(
            src_ref=src, dst_ref=dst, send_sem=ssem, recv_sem=rsem,
            device_id=to, device_id_type=pl.DeviceIdType.MESH,
        )

    def landed(ref, sem):
        remote(ref, ref, sem, sem, peer(1)).wait_recv()

    def sent(ref, sem):
        remote(ref, ref, sem, sem, peer(1)).wait_send()

    barrier = pltpu.get_barrier_semaphore()
    for off in range(1, n):
        pl.semaphore_signal(
            barrier, inc=1, device_id=peer(off), device_id_type=pl.DeviceIdType.MESH
        )
    icopies = [
        pltpu.make_async_copy(src, dst, isem.at[i])
        for i, (src, dst) in enumerate((
            (lens_hbm, lens_ref), (owner_hbm, owner_ref), (slot_hbm, slot_ref), (q_hbm, q_ref),
        ))
    ]
    for copy in icopies:
        copy.start()
    kcopies = [pltpu.make_async_copy(k_hbm.at[:, h], kbuf.at[h], ksem.at[h]) for h in range(kv)]
    vcopies = [pltpu.make_async_copy(v_hbm.at[:, h], vbuf.at[h], vsem.at[h]) for h in range(kv)]

    for copy in icopies:
        copy.wait()
    loads = kcopies + vcopies
    for copy in loads[:DEPTH]:
        copy.start()
    span = owner_ref.shape[1]
    row = iota((rows, span), 0)
    length = jnp.zeros((rows, span), jnp.int32)
    for r in range(rows):
        length = jnp.where(row == r, lens_ref[r], length)
    live = jnp.clip(length - iota((rows, span), 1) * tokens, 0, tokens)
    live_f = live.astype(F32)
    owner = owner_ref[...]
    slot = slot_ref[...]
    ones = jnp.ones((8, span), BF16)
    slot_id = iota((pool, span), 0)
    for off in range(n):
        there = lax.rem(me + off, n)
        key = jnp.where((owner == there) & (live > 0), slot, -1)
        acc_live = jnp.zeros((pool, span), F32)
        acc_req = jnp.zeros((pool, span), F32)
        for r in range(rows):
            hit = slot_id == key[r : r + 1, :]
            acc_live = jnp.where(hit, live_f[r : r + 1, :], acc_live)
            acc_req = jnp.where(hit, float(r + 1), acc_req)
        t_live = lax.dot_general(ones, acc_live.astype(BF16), NT, preferred_element_type=F32)
        t_req = lax.dot_general(ones, acc_req.astype(BF16), NT, preferred_element_type=F32)
        table = (t_req * CODE + t_live)[0:1, :]
        if lanes > pool:
            table = jnp.concatenate([table, jnp.zeros((1, lanes - pool), F32)], axis=1)
        if off == 0:
            trecv[0] = table
        else:
            tsend[off] = table

    queries = q_ref[...].astype(F32).reshape(rows, kv, group, width)
    for h in range(kv):
        qall[h, 0:block, :] = queries[:, h].reshape(block, width).astype(BF16)

    pl.semaphore_wait(barrier, n - 1)
    tcopies = {}
    qcopies = {}
    for off in range(1, n):
        tcopies[off] = remote(
            tsend.at[off], trecv.at[off], tss, trs, peer(off)
        )
        tcopies[off].start()
    for h in range(kv):
        for off in range(1, n):
            qcopies[h, off] = remote(
                qall.at[h, pl.ds(0, block)],
                qall.at[h, pl.ds(off * block, block)],
                qss, qrs.at[h], peer(off),
            )

    def send(first, last):
        for h in range(first, last):
            for off in range(1, n):
                qcopies[h, off].start()

    early = lax.axis_index("rep") == 0

    @pl.when(early)
    def _():
        send(0, kv)

    step = math.gcd(pool, 16)
    for h in range(kv):
        kcopies[h].wait()
        for copy in loads[DEPTH + h :] if h == kv - 1 else loads[DEPTH + h : DEPTH + h + 1]:
            copy.start()

        def turn(i, carry):
            for u in range(step):
                kbuf[h, i * step + u] = kbuf[h, i * step + u].T
            return carry

        lax.fori_loop(0, pool // step, turn, 0)
        if h == LATE:

            @pl.when(jnp.logical_not(early))
            def _():
                send(0, kv)

    landed(trecv.at[pl.ds(1, n - 1)], trs)
    live_row = jnp.zeros((1, lanes), F32)
    req_row = jnp.zeros((1, lanes), F32)
    for off in range(n):
        t = trecv[off]
        request = jnp.floor(t * (1.0 / CODE))
        live_row = live_row + (t - request * CODE)
        req_row = req_row + jnp.where(request > 0.0, request + float(off * rows), 0.0)
    pg = pool * group
    spread = jnp.where(iota((pg, lanes), 0) // group == iota((pg, lanes), 1), 1.0, 0.0)
    spread = spread.astype(BF16)
    liveb[...] = lax.dot_general(
        spread, jnp.broadcast_to(live_row, (128, lanes)).astype(BF16), NT,
        preferred_element_type=F32,
    )
    reqb[...] = lax.dot_general(
        spread, jnp.broadcast_to(req_row, (128, lanes)).astype(BF16), NT,
        preferred_element_type=F32,
    )
    same = iota((pg, 128), 0) % group == iota((pg, 128), 1) % group
    for c in range(n * block // 128):
        want = ((iota((pg, 128), 1) + c * 128) // group + 1).astype(F32)
        mt[:, c * 128 : (c + 1) * 128] = jnp.where(
            same & (reqb[...] == want), 1.0, 0.0
        ).astype(BF16)
    spread_t = jnp.where(iota((lanes, pg), 0) == iota((lanes, pg), 1) // group, 1.0, 0.0)
    req_wide = jnp.dot(
        jnp.broadcast_to(req_row, (8, lanes)).astype(BF16), spread_t.astype(BF16),
        preferred_element_type=F32,
    )[0:1, :]
    same_t = iota((block, pg), 0) % group == iota((block, pg), 1) % group
    for off in range(n):
        want = (iota((block, pg), 0) // group + (off * rows + 1)).astype(F32)
        m[off * block : (off + 1) * block, :] = jnp.where(
            same_t & (req_wide == want), 1.0, 0.0
        ).astype(BF16)

    lane_f = iota((group, 128), 1).astype(F32)
    lane = iota((group, 128), 1)
    pair = 2 * group
    pairs = pool // 2
    ahead = min(8, pairs)
    tops = [jnp.full((group, 128), MASKED, F32) for _ in range(kv)]
    sums = [jnp.zeros((group, 128), F32) for _ in range(kv)]
    ocopies = {}
    scopies = {}

    def gather(h):
        landed(qall.at[h, pl.ds(block, (n - 1) * block)], qrs.at[h])
        half = pool * group // 2
        for u in range(2):
            at = slice(u * half, (u + 1) * half)
            qslot[h % 2, at, :] = jnp.dot(
                mt[at, :], qall[h], preferred_element_type=F32
            ).astype(BF16)

    def score(h, i):
        keys = jnp.concatenate([kbuf[h, 2 * i], kbuf[h, 2 * i + 1]], axis=1)
        s = jnp.dot(
            qslot[h % 2, i * pair : (i + 1) * pair, :], keys, preferred_element_type=F32
        )
        for u in range(2):
            at = slice((2 * i + u) * group, (2 * i + u + 1) * group)
            x = s[u * group : (u + 1) * group, u * tokens : (u + 1) * tokens]
            x = jnp.where(lane_f < liveb[at, :], x * scale, MASKED)
            wbuf[h % 2, at, :] = x
            pm = jnp.max(x, axis=1, keepdims=True)
            tops[h] = jnp.maximum(
                tops[h], jnp.where(reqb[at, :] == lane_f + 1.0, pm, MASKED)
            )

    def weigh(h, i):
        weights = []
        for u in range(2):
            at = slice((2 * i + u) * group, (2 * i + u + 1) * group)
            mine = reqb[at, :] == lane_f + 1.0
            rm = jnp.max(jnp.where(mine, tops[h], MASKED), axis=1, keepdims=True)
            w = jnp.exp2(wbuf[h % 2, at, :] - rm)
            sums[h] = sums[h] + jnp.where(mine, jnp.sum(w, axis=1, keepdims=True), 0.0)
            weights.append(w)
        both = jnp.concatenate([vbuf[h, 2 * i], vbuf[h, 2 * i + 1]], axis=1)
        out = jnp.dot(
            jnp.concatenate(weights, axis=0).astype(BF16), both, preferred_element_type=F32
        )
        ohi[i * pair : (i + 1) * pair, :] = jnp.concatenate(
            [out[u * group : (u + 1) * group, u * width : (u + 1) * width] for u in range(2)],
            axis=0,
        ).astype(BF16)

    def statistics():
        for off in range(n):
            stat = jnp.zeros((group, 128), F32)
            for g in range(kv):
                for j, x in enumerate((tops[g], sums[g])):
                    at = (2 * g + j) * rows
                    shift = (at - off * rows) % 128
                    y = pltpu.roll(x, shift, 1) if shift else x
                    stat = jnp.where((lane >= at) & (lane < at + rows), y, stat)
            if off == 0:
                srecv[0] = stat
            else:
                ssend[off] = stat
                scopies[off] = remote(
                    ssend.at[off], srecv.at[off], sss, srs, source(off)
                )
                scopies[off].start()

    def finish(h):
        if h == kv - 1:
            statistics()
        osend[h] = jnp.dot(m[...], ohi[...], preferred_element_type=F32).astype(BF16)
        for off in range(1, n):
            ocopies[h, off] = remote(
                osend.at[h, pl.ds(off * block, block)], orecv.at[h, off],
                oss, ors.at[h], source(off),
            )
            ocopies[h, off].start()

    gather(0)
    for i in range(pairs):
        score(0, i)
    for h in range(kv):
        vcopies[h].wait()
        more = h + 1 < kv
        if more:
            gather(h + 1)
        for i in range(pairs + ahead):
            if more and i >= ahead:
                score(h + 1, i - ahead)
            if i < pairs:
                weigh(h, i)
            if i == pairs - 1:
                finish(h)

    landed(srecv.at[pl.ds(1, n - 1)], srs)
    stats = [srecv[off] for off in range(n)]
    best = functools.reduce(jnp.maximum, stats)
    factors = [jnp.exp2(x - best) for x in stats]
    whole = functools.reduce(
        jnp.add, [f * pltpu.roll(x, 128 - rows, 1) for f, x in zip(factors, stats)]
    )
    factors = [f / whole for f in factors]
    parts = []
    for h in range(kv):
        landed(orecv.at[h, pl.ds(1, n - 1)], ors.at[h])
        gathered = []
        for off in range(n):
            got = orecv[h, off] if off else osend[h, 0:block, :]
            gathered.append(got.astype(F32).reshape(rows, group, width))
        per_row = []
        for r in range(rows):
            at = 2 * h * rows + r
            total = factors[0][:, at : at + 1] * gathered[0][r]
            for off in range(1, n):
                total = total + factors[off][:, at : at + 1] * gathered[off][r]
            per_row.append(total)
        parts.append(per_row)
    for r in range(rows):
        out_ref[r] = jnp.concatenate([parts[h][r] for h in range(kv)], axis=0).astype(BF16)

    sent(trecv.at[pl.ds(1, n - 1)], tss)
    sent(qall.at[:, pl.ds(block, (n - 1) * block)], qss)
    sent(osend.at[:, pl.ds(block, (n - 1) * block)], oss)
    sent(srecv.at[pl.ds(1, n - 1)], sss)


def on_device(n, queries, page_owner, page_slot, lengths, keys, values):
    pool, kv, tokens, width = keys.shape
    rows, heads, _ = queries.shape
    group = heads // kv
    block = rows * group
    pg = pool * group
    lanes = -(-pool // 128) * 128
    dma = pltpu.SemaphoreType.DMA
    vmem = pl.BlockSpec(memory_space=pltpu.VMEM)
    return pl.pallas_call(
        functools.partial(kernel, n),
        out_shape=pltpu.VMEM(queries.shape, BF16),
        in_specs=[pl.BlockSpec(memory_space=pl.ANY)] * 6,
        out_specs=vmem,
        scratch_shapes=[
            pltpu.SMEM(lengths.shape, jnp.int32),
            pltpu.VMEM(queries.shape, BF16),
            pltpu.VMEM(page_owner.shape, jnp.int32),
            pltpu.VMEM(page_slot.shape, jnp.int32),
            pltpu.VMEM((kv, pool, tokens, width), BF16),
            pltpu.VMEM((kv, pool, tokens, width), BF16),
            pltpu.VMEM((kv, n * block, width), BF16),
            pltpu.VMEM((n, 1, lanes), F32),
            pltpu.VMEM((n, 1, lanes), F32),
            pltpu.VMEM((pg, 128), F32),
            pltpu.VMEM((pg, 128), F32),
            pltpu.VMEM((pg, n * block), BF16),
            pltpu.VMEM((n * block, pg), BF16),
            pltpu.VMEM((2, pg, width), BF16),
            pltpu.VMEM((2, pg, tokens), F32),
            pltpu.VMEM((pg, width), BF16),
            pltpu.VMEM((kv, n * block, width), BF16),
            pltpu.VMEM((kv, n, block, width), BF16),
            pltpu.VMEM((n, group, 128), F32),
            pltpu.VMEM((n, group, 128), F32),
            dma((4,)), dma((kv,)), dma((kv,)),
            dma, dma,
            dma, dma((kv,)),
            dma, dma((kv,)),
            dma, dma,
        ],
        compiler_params=pltpu.CompilerParams(
            collective_id=0, has_side_effects=True, vmem_limit_bytes=66977792
        ),
        name="paged",
    )(lengths, queries, page_owner, page_slot, keys, values)


def solution(mesh):
    placed = (
        P(("groups", "seq", "rep"), "head", None),
        P(("groups", "seq", "rep"), None),
        P(("groups", "seq", "rep"), None),
        P(("groups", "seq", "rep")),
        P(("groups", "seq", "rep"), "head", None, None),
        P(("groups", "seq", "rep"), "head", None, None),
    )
    return jax.shard_map(
        functools.partial(on_device, mesh.shape["seq"]),
        mesh=mesh,
        in_specs=placed,
        out_specs=P(("groups", "seq", "rep"), "head", None),
        check_vma=False,
    )
```

```python
import functools
import math

import jax
import jax.numpy as jnp
from jax import lax
from jax.experimental import pallas as pl
from jax.experimental.pallas import tpu as pltpu
from jax.sharding import PartitionSpec as P

MASKED = -1e30
CODE = 256.0
LATE = 1
DEPTH = 3
F32 = jnp.float32
BF16 = jnp.bfloat16
NT = (((1,), (1,)), ((), ()))


def iota(shape, dim):
    return lax.broadcasted_iota(jnp.int32, shape, dim)


def kernel(
    n, lens_hbm, q_hbm, owner_hbm, slot_hbm, k_hbm, v_hbm, out_ref,
    lens_ref, q_ref, owner_ref, slot_ref, kbuf, vbuf, qall, tsend, trecv, liveb, reqb, mt, m, qslot, wbuf, ohi,
    osend, orecv, ssend, srecv,
    isem, ksem, vsem, tss, trs, qss, qrs, oss, ors, sss, srs,
):
    pool, kv, tokens, width = k_hbm.shape
    rows = q_hbm.shape[0]
    group = q_hbm.shape[1] // kv
    block = rows * group
    lanes = trecv.shape[2]
    scale = math.log2(math.e) / math.sqrt(width)
    me = lax.axis_index("seq")

    def peer(off):
        return {"seq": lax.rem(me + off, n)}

    def source(off):
        return {"seq": lax.rem(me + n - off, n)}

    def remote(src, dst, ssem, rsem, to):
        return pltpu.make_async_remote_copy(
            src_ref=src, dst_ref=dst, send_sem=ssem, recv_sem=rsem,
            device_id=to, device_id_type=pl.DeviceIdType.MESH,
        )

    def landed(ref, sem):
        remote(ref, ref, sem, sem, peer(1)).wait_recv()

    def sent(ref, sem):
        remote(ref, ref, sem, sem, peer(1)).wait_send()

    barrier = pltpu.get_barrier_semaphore()
    for off in range(1, n):
        pl.semaphore_signal(
            barrier, inc=1, device_id=peer(off), device_id_type=pl.DeviceIdType.MESH
        )
    icopies = [
        pltpu.make_async_copy(src, dst, isem.at[i])
        for i, (src, dst) in enumerate((
            (lens_hbm, lens_ref), (owner_hbm, owner_ref), (slot_hbm, slot_ref), (q_hbm, q_ref),
        ))
    ]
    for copy in icopies:
        copy.start()
    kcopies = [pltpu.make_async_copy(k_hbm.at[:, h], kbuf.at[h], ksem.at[h]) for h in range(kv)]
    vcopies = [pltpu.make_async_copy(v_hbm.at[:, h], vbuf.at[h], vsem.at[h]) for h in range(kv)]

    for copy in icopies:
        copy.wait()
    loads = kcopies + vcopies
    for copy in loads[:DEPTH]:
        copy.start()
    span = owner_ref.shape[1]
    row = iota((rows, span), 0)
    length = jnp.zeros((rows, span), jnp.int32)
    for r in range(rows):
        length = jnp.where(row == r, lens_ref[r], length)
    live = jnp.clip(length - iota((rows, span), 1) * tokens, 0, tokens)
    live_f = live.astype(F32)
    owner = owner_ref[...]
    slot = slot_ref[...]
    ones = jnp.ones((8, span), BF16)
    slot_id = iota((pool, span), 0)
    for off in range(n):
        there = lax.rem(me + off, n)
        key = jnp.where((owner == there) & (live > 0), slot, -1)
        acc_live = jnp.zeros((pool, span), F32)
        acc_req = jnp.zeros((pool, span), F32)
        for r in range(rows):
            hit = slot_id == key[r : r + 1, :]
            acc_live = jnp.where(hit, live_f[r : r + 1, :], acc_live)
            acc_req = jnp.where(hit, float(r + 1), acc_req)
        t_live = lax.dot_general(ones, acc_live.astype(BF16), NT, preferred_element_type=F32)
        t_req = lax.dot_general(ones, acc_req.astype(BF16), NT, preferred_element_type=F32)
        table = (t_req * CODE + t_live)[0:1, :]
        if lanes > pool:
            table = jnp.concatenate([table, jnp.zeros((1, lanes - pool), F32)], axis=1)
        if off == 0:
            trecv[0] = table
        else:
            tsend[off] = table

    queries = q_ref[...].astype(F32).reshape(rows, kv, group, width)
    for h in range(kv):
        qall[h, 0:block, :] = queries[:, h].reshape(block, width).astype(BF16)

    pl.semaphore_wait(barrier, n - 1)
    tcopies = {}
    qcopies = {}
    for off in range(1, n):
        tcopies[off] = remote(
            tsend.at[off], trecv.at[off], tss, trs, peer(off)
        )
        tcopies[off].start()
    for h in range(kv):
        for off in range(1, n):
            qcopies[h, off] = remote(
                qall.at[h, pl.ds(0, block)],
                qall.at[h, pl.ds(off * block, block)],
                qss, qrs.at[h], peer(off),
            )

    def send(first, last):
        for h in range(first, last):
            for off in range(1, n):
                qcopies[h, off].start()

    early = lax.axis_index("rep") == 0

    @pl.when(early)
    def _():
        send(0, kv)

    step = math.gcd(pool, 16)
    for h in range(kv):
        kcopies[h].wait()
        for copy in loads[DEPTH + h :] if h == kv - 1 else loads[DEPTH + h : DEPTH + h + 1]:
            copy.start()

        def turn(i, carry):
            for u in range(step):
                kbuf[h, i * step + u] = kbuf[h, i * step + u].T
            return carry

        lax.fori_loop(0, pool // step, turn, 0)
        if h == LATE:

            @pl.when(jnp.logical_not(early))
            def _():
                send(0, kv)

    landed(trecv.at[pl.ds(1, n - 1)], trs)
    live_row = jnp.zeros((1, lanes), F32)
    req_row = jnp.zeros((1, lanes), F32)
    for off in range(n):
        t = trecv[off]
        request = jnp.floor(t * (1.0 / CODE))
        live_row = live_row + (t - request * CODE)
        req_row = req_row + jnp.where(request > 0.0, request + float(off * rows), 0.0)
    pg = pool * group
    spread = jnp.where(iota((pg, lanes), 0) // group == iota((pg, lanes), 1), 1.0, 0.0)
    spread = spread.astype(BF16)
    liveb[...] = lax.dot_general(
        spread, jnp.broadcast_to(live_row, (128, lanes)).astype(BF16), NT,
        preferred_element_type=F32,
    )
    reqb[...] = lax.dot_general(
        spread, jnp.broadcast_to(req_row, (128, lanes)).astype(BF16), NT,
        preferred_element_type=F32,
    )
    same = iota((pg, 128), 0) % group == iota((pg, 128), 1) % group
    for c in range(n * block // 128):
        want = ((iota((pg, 128), 1) + c * 128) // group + 1).astype(F32)
        mt[:, c * 128 : (c + 1) * 128] = jnp.where(
            same & (reqb[...] == want), 1.0, 0.0
        ).astype(BF16)
    spread_t = jnp.where(iota((lanes, pg), 0) == iota((lanes, pg), 1) // group, 1.0, 0.0)
    req_wide = jnp.dot(
        jnp.broadcast_to(req_row, (8, lanes)).astype(BF16), spread_t.astype(BF16),
        preferred_element_type=F32,
    )[0:1, :]
    same_t = iota((block, pg), 0) % group == iota((block, pg), 1) % group
    for off in range(n):
        want = (iota((block, pg), 0) // group + (off * rows + 1)).astype(F32)
        m[off * block : (off + 1) * block, :] = jnp.where(
            same_t & (req_wide == want), 1.0, 0.0
        ).astype(BF16)

    lane_f = iota((group, 128), 1).astype(F32)
    lane = iota((group, 128), 1)
    pair = 2 * group
    pairs = pool // 2
    ahead = min(8, pairs)
    tops = [jnp.full((group, 128), MASKED, F32) for _ in range(kv)]
    sums = [jnp.zeros((group, 128), F32) for _ in range(kv)]
    ocopies = {}

    def gather(h):
        landed(qall.at[h, pl.ds(block, (n - 1) * block)], qrs.at[h])
        half = pool * group // 2
        for u in range(2):
            at = slice(u * half, (u + 1) * half)
            qslot[h % 2, at, :] = jnp.dot(
                mt[at, :], qall[h], preferred_element_type=F32
            ).astype(BF16)

    def score(h, i):
        keys = jnp.concatenate([kbuf[h, 2 * i], kbuf[h, 2 * i + 1]], axis=1)
        s = jnp.dot(
            qslot[h % 2, i * pair : (i + 1) * pair, :], keys, preferred_element_type=F32
        )
        for u in range(2):
            at = slice((2 * i + u) * group, (2 * i + u + 1) * group)
            x = s[u * group : (u + 1) * group, u * tokens : (u + 1) * tokens]
            x = jnp.where(lane_f < liveb[at, :], x * scale, MASKED)
            wbuf[h % 2, at, :] = x
            pm = jnp.max(x, axis=1, keepdims=True)
            tops[h] = jnp.maximum(
                tops[h], jnp.where(reqb[at, :] == lane_f + 1.0, pm, MASKED)
            )

    def weigh(h, i):
        weights = []
        for u in range(2):
            at = slice((2 * i + u) * group, (2 * i + u + 1) * group)
            mine = reqb[at, :] == lane_f + 1.0
            rm = jnp.max(jnp.where(mine, tops[h], MASKED), axis=1, keepdims=True)
            w = jnp.exp2(wbuf[h % 2, at, :] - rm)
            sums[h] = sums[h] + jnp.where(mine, jnp.sum(w, axis=1, keepdims=True), 0.0)
            weights.append(w)
        both = jnp.concatenate([vbuf[h, 2 * i], vbuf[h, 2 * i + 1]], axis=1)
        out = jnp.dot(
            jnp.concatenate(weights, axis=0).astype(BF16), both, preferred_element_type=F32
        )
        ohi[i * pair : (i + 1) * pair, :] = jnp.concatenate(
            [out[u * group : (u + 1) * group, u * width : (u + 1) * width] for u in range(2)],
            axis=0,
        ).astype(BF16)

    wide = 2 * rows
    place = lane // wide == -iota((group, 128), 0) % (128 // wide)

    def shifted(x, by):
        return pltpu.roll(x, by % 128, 1) if by % 128 else x

    def statistics(h):
        for off in range(n):
            stat = jnp.where(lane < rows, shifted(tops[h], -off * rows), 0.0)
            total = shifted(sums[h], (1 - off) * rows)
            stat = jnp.where((lane >= rows) & (lane < wide), total, stat)
            by = wide
            while by < 128:
                stat = stat + shifted(stat, by)
                by *= 2
            stat = jnp.sum(jnp.where(place, stat, 0.0), axis=0, keepdims=True)
            if off == 0:
                srecv[h, 0] = stat
            else:
                ssend[h, off] = stat
                remote(
                    ssend.at[h, off], srecv.at[h, off], sss, srs.at[h], source(off)
                ).start()

    def finish(h):
        statistics(h)
        osend[h] = jnp.dot(m[...], ohi[...], preferred_element_type=F32).astype(BF16)
        for off in range(1, n):
            ocopies[h, off] = remote(
                osend.at[h, pl.ds(off * block, block)], orecv.at[h, off],
                oss, ors.at[h], source(off),
            )
            ocopies[h, off].start()

    gather(0)
    for i in range(pairs):
        score(0, i)
    for h in range(kv):
        vcopies[h].wait()
        more = h + 1 < kv
        if more:
            gather(h + 1)
        for i in range(pairs + ahead):
            if more and i >= ahead:
                score(h + 1, i - ahead)
            if i < pairs:
                weigh(h, i)
            if i == pairs - 1:
                finish(h)

    for h in range(kv):
        landed(srecv.at[h, pl.ds(1, n - 1)], srs.at[h])
        stats = [
            pltpu.roll(
                jnp.broadcast_to(srecv[h, off], (group, 128)),
                0, 1, stride=wide, stride_axis=0,
            )
            for off in range(n)
        ]
        best = functools.reduce(jnp.maximum, stats)
        factors = [jnp.exp2(x - best) for x in stats]
        whole = functools.reduce(
            jnp.add, [f * pltpu.roll(x, 128 - rows, 1) for f, x in zip(factors, stats)]
        )
        factors = [f / whole for f in factors]
        landed(orecv.at[h, pl.ds(1, n - 1)], ors.at[h])
        gathered = []
        for off in range(n):
            got = orecv[h, off] if off else osend[h, 0:block, :]
            gathered.append(got.astype(F32).reshape(rows, group, width))
        for r in range(rows):
            total = factors[0][:, r : r + 1] * gathered[0][r]
            for off in range(1, n):
                total = total + factors[off][:, r : r + 1] * gathered[off][r]
            out_ref[r, h * group : (h + 1) * group, :] = total.astype(BF16)

    sent(trecv.at[pl.ds(1, n - 1)], tss)
    sent(qall.at[:, pl.ds(block, (n - 1) * block)], qss)
    sent(osend.at[:, pl.ds(block, (n - 1) * block)], oss)
    sent(srecv.at[:, pl.ds(1, n - 1)], sss)


def on_device(n, queries, page_owner, page_slot, lengths, keys, values):
    pool, kv, tokens, width = keys.shape
    rows, heads, _ = queries.shape
    group = heads // kv
    block = rows * group
    pg = pool * group
    lanes = -(-pool // 128) * 128
    dma = pltpu.SemaphoreType.DMA
    vmem = pl.BlockSpec(memory_space=pltpu.VMEM)
    return pl.pallas_call(
        functools.partial(kernel, n),
        out_shape=pltpu.VMEM(queries.shape, BF16),
        in_specs=[pl.BlockSpec(memory_space=pl.ANY)] * 6,
        out_specs=vmem,
        scratch_shapes=[
            pltpu.SMEM(lengths.shape, jnp.int32),
            pltpu.VMEM(queries.shape, BF16),
            pltpu.VMEM(page_owner.shape, jnp.int32),
            pltpu.VMEM(page_slot.shape, jnp.int32),
            pltpu.VMEM((kv, pool, tokens, width), BF16),
            pltpu.VMEM((kv, pool, tokens, width), BF16),
            pltpu.VMEM((kv, n * block, width), BF16),
            pltpu.VMEM((n, 1, lanes), F32),
            pltpu.VMEM((n, 1, lanes), F32),
            pltpu.VMEM((pg, 128), F32),
            pltpu.VMEM((pg, 128), F32),
            pltpu.VMEM((pg, n * block), BF16),
            pltpu.VMEM((n * block, pg), BF16),
            pltpu.VMEM((2, pg, width), BF16),
            pltpu.VMEM((2, pg, tokens), F32),
            pltpu.VMEM((pg, width), BF16),
            pltpu.VMEM((kv, n * block, width), BF16),
            pltpu.VMEM((kv, n, block, width), BF16),
            pltpu.VMEM((kv, n, 1, 128), F32),
            pltpu.VMEM((kv, n, 1, 128), F32),
            dma((4,)), dma((kv,)), dma((kv,)),
            dma, dma,
            dma, dma((kv,)),
            dma, dma((kv,)),
            dma, dma((kv,)),
        ],
        compiler_params=pltpu.CompilerParams(
            collective_id=0, has_side_effects=True, vmem_limit_bytes=66977792
        ),
        name="paged",
    )(lengths, queries, page_owner, page_slot, keys, values)


def solution(mesh):
    placed = (
        P(("groups", "seq", "rep"), "head", None),
        P(("groups", "seq", "rep"), None),
        P(("groups", "seq", "rep"), None),
        P(("groups", "seq", "rep")),
        P(("groups", "seq", "rep"), "head", None, None),
        P(("groups", "seq", "rep"), "head", None, None),
    )
    return jax.shard_map(
        functools.partial(on_device, mesh.shape["seq"]),
        mesh=mesh,
        in_specs=placed,
        out_specs=P(("groups", "seq", "rep"), "head", None),
        check_vma=False,
    )
```

```python
import functools
import math

import jax
import jax.numpy as jnp
from jax import lax
from jax.experimental import pallas as pl
from jax.experimental.pallas import tpu as pltpu
from jax.sharding import PartitionSpec as P

MASKED = -1e30
CODE = 256.0
LATE = 1
DEPTH = 3
F32 = jnp.float32
BF16 = jnp.bfloat16
NT = (((1,), (1,)), ((), ()))


def iota(shape, dim):
    return lax.broadcasted_iota(jnp.int32, shape, dim)


def kernel(
    n, lens_hbm, q_hbm, owner_hbm, slot_hbm, k_hbm, v_hbm, out_ref,
    lens_ref, q_ref, owner_ref, slot_ref, kbuf, vbuf, qall, tsend, trecv, liveb, reqb, mt, m, qslot, wbuf, ohi,
    osend, orecv, ssend, srecv,
    isem, ksem, vsem, tss, trs, qss, qrs, oss, ors, sss, srs,
):
    pool, kv, tokens, width = k_hbm.shape
    rows = q_hbm.shape[0]
    group = q_hbm.shape[1] // kv
    block = rows * group
    lanes = trecv.shape[2]
    scale = math.log2(math.e) / math.sqrt(width)
    me = lax.axis_index("seq")

    def peer(off):
        return {"seq": lax.rem(me + off, n)}

    def source(off):
        return {"seq": lax.rem(me + n - off, n)}

    def remote(src, dst, ssem, rsem, to):
        return pltpu.make_async_remote_copy(
            src_ref=src, dst_ref=dst, send_sem=ssem, recv_sem=rsem,
            device_id=to, device_id_type=pl.DeviceIdType.MESH,
        )

    def landed(ref, sem):
        remote(ref, ref, sem, sem, peer(1)).wait_recv()

    def sent(ref, sem):
        remote(ref, ref, sem, sem, peer(1)).wait_send()

    barrier = pltpu.get_barrier_semaphore()
    for off in range(1, n):
        pl.semaphore_signal(
            barrier, inc=1, device_id=peer(off), device_id_type=pl.DeviceIdType.MESH
        )
    icopies = [
        pltpu.make_async_copy(src, dst, isem.at[i])
        for i, (src, dst) in enumerate((
            (lens_hbm, lens_ref), (owner_hbm, owner_ref), (slot_hbm, slot_ref), (q_hbm, q_ref),
        ))
    ]
    for copy in icopies:
        copy.start()
    kcopies = [pltpu.make_async_copy(k_hbm.at[:, h], kbuf.at[h], ksem.at[h]) for h in range(kv)]
    vcopies = [pltpu.make_async_copy(v_hbm.at[:, h], vbuf.at[h], vsem.at[h]) for h in range(kv)]

    for copy in icopies:
        copy.wait()
    loads = kcopies + vcopies
    for copy in loads[:DEPTH]:
        copy.start()
    span = owner_ref.shape[1]
    row = iota((rows, span), 0)
    length = jnp.zeros((rows, span), jnp.int32)
    for r in range(rows):
        length = jnp.where(row == r, lens_ref[r], length)
    live = jnp.clip(length - iota((rows, span), 1) * tokens, 0, tokens)
    live_f = live.astype(F32)
    owner = owner_ref[...]
    slot = slot_ref[...]
    ones = jnp.ones((8, span), BF16)
    slot_id = iota((pool, span), 0)
    for off in range(n):
        there = lax.rem(me + off, n)
        key = jnp.where((owner == there) & (live > 0), slot, -1)
        acc_live = jnp.zeros((pool, span), F32)
        acc_req = jnp.zeros((pool, span), F32)
        for r in range(rows):
            hit = slot_id == key[r : r + 1, :]
            acc_live = jnp.where(hit, live_f[r : r + 1, :], acc_live)
            acc_req = jnp.where(hit, float(r + 1), acc_req)
        t_live = lax.dot_general(ones, acc_live.astype(BF16), NT, preferred_element_type=F32)
        t_req = lax.dot_general(ones, acc_req.astype(BF16), NT, preferred_element_type=F32)
        table = (t_req * CODE + t_live)[0:1, :]
        if lanes > pool:
            table = jnp.concatenate([table, jnp.zeros((1, lanes - pool), F32)], axis=1)
        if off == 0:
            trecv[0] = table
        else:
            tsend[off] = table

    queries = q_ref[...].astype(F32).reshape(rows, kv, group, width)
    for h in range(kv):
        qall[h, 0:block, :] = queries[:, h].reshape(block, width).astype(BF16)

    pl.semaphore_wait(barrier, n - 1)
    tcopies = {}
    qcopies = {}
    for off in range(1, n):
        tcopies[off] = remote(
            tsend.at[off], trecv.at[off], tss, trs, peer(off)
        )
        tcopies[off].start()
    for h in range(kv):
        for off in range(1, n):
            qcopies[h, off] = remote(
                qall.at[h, pl.ds(0, block)],
                qall.at[h, pl.ds(off * block, block)],
                qss, qrs.at[h], peer(off),
            )

    def send(first, last):
        for h in range(first, last):
            for off in range(1, n):
                qcopies[h, off].start()

    early = lax.axis_index("rep") == 0

    @pl.when(early)
    def _():
        send(0, kv)

    step = math.gcd(pool, 16)
    for h in range(kv):
        kcopies[h].wait()
        for copy in loads[DEPTH + h :] if h == kv - 1 else loads[DEPTH + h : DEPTH + h + 1]:
            copy.start()

        def turn(i, carry):
            for u in range(step):
                kbuf[h, i * step + u] = kbuf[h, i * step + u].T
            return carry

        lax.fori_loop(0, pool // step, turn, 0)
        if h == 0:

            @pl.when(jnp.logical_not(early))
            def _():
                send(0, 1)

        if h == 2:

            @pl.when(jnp.logical_not(early))
            def _():
                send(1, kv)


    landed(trecv.at[pl.ds(1, n - 1)], trs)
    live_row = jnp.zeros((1, lanes), F32)
    req_row = jnp.zeros((1, lanes), F32)
    for off in range(n):
        t = trecv[off]
        request = jnp.floor(t * (1.0 / CODE))
        live_row = live_row + (t - request * CODE)
        req_row = req_row + jnp.where(request > 0.0, request + float(off * rows), 0.0)
    pg = pool * group
    spread = jnp.where(iota((pg, lanes), 0) // group == iota((pg, lanes), 1), 1.0, 0.0)
    spread = spread.astype(BF16)
    liveb[...] = lax.dot_general(
        spread, jnp.broadcast_to(live_row, (128, lanes)).astype(BF16), NT,
        preferred_element_type=F32,
    )
    reqb[...] = lax.dot_general(
        spread, jnp.broadcast_to(req_row, (128, lanes)).astype(BF16), NT,
        preferred_element_type=F32,
    )
    same = iota((pg, 128), 0) % group == iota((pg, 128), 1) % group
    for c in range(n * block // 128):
        want = ((iota((pg, 128), 1) + c * 128) // group + 1).astype(F32)
        mt[:, c * 128 : (c + 1) * 128] = jnp.where(
            same & (reqb[...] == want), 1.0, 0.0
        ).astype(BF16)
    spread_t = jnp.where(iota((lanes, pg), 0) == iota((lanes, pg), 1) // group, 1.0, 0.0)
    req_wide = jnp.dot(
        jnp.broadcast_to(req_row, (8, lanes)).astype(BF16), spread_t.astype(BF16),
        preferred_element_type=F32,
    )[0:1, :]
    same_t = iota((block, pg), 0) % group == iota((block, pg), 1) % group
    for off in range(n):
        want = (iota((block, pg), 0) // group + (off * rows + 1)).astype(F32)
        m[off * block : (off + 1) * block, :] = jnp.where(
            same_t & (req_wide == want), 1.0, 0.0
        ).astype(BF16)

    lane_f = iota((group, 128), 1).astype(F32)
    lane = iota((group, 128), 1)
    pair = 2 * group
    pairs = pool // 2
    ahead = min(8, pairs)
    tops = [jnp.full((group, 128), MASKED, F32) for _ in range(kv)]
    sums = [jnp.zeros((group, 128), F32) for _ in range(kv)]
    ocopies = {}

    def gather(h):
        landed(qall.at[h, pl.ds(block, (n - 1) * block)], qrs.at[h])
        half = pool * group // 2
        for u in range(2):
            at = slice(u * half, (u + 1) * half)
            qslot[h % 2, at, :] = jnp.dot(
                mt[at, :], qall[h], preferred_element_type=F32
            ).astype(BF16)

    def score(h, i):
        keys = jnp.concatenate([kbuf[h, 2 * i], kbuf[h, 2 * i + 1]], axis=1)
        s = jnp.dot(
            qslot[h % 2, i * pair : (i + 1) * pair, :], keys, preferred_element_type=F32
        )
        for u in range(2):
            at = slice((2 * i + u) * group, (2 * i + u + 1) * group)
            x = s[u * group : (u + 1) * group, u * tokens : (u + 1) * tokens]
            x = jnp.where(lane_f < liveb[at, :], x * scale, MASKED)
            wbuf[h % 2, at, :] = x
            pm = jnp.max(x, axis=1, keepdims=True)
            tops[h] = jnp.maximum(
                tops[h], jnp.where(reqb[at, :] == lane_f + 1.0, pm, MASKED)
            )

    def weigh(h, i):
        weights = []
        for u in range(2):
            at = slice((2 * i + u) * group, (2 * i + u + 1) * group)
            mine = reqb[at, :] == lane_f + 1.0
            rm = jnp.max(jnp.where(mine, tops[h], MASKED), axis=1, keepdims=True)
            w = jnp.exp2(wbuf[h % 2, at, :] - rm)
            sums[h] = sums[h] + jnp.where(mine, jnp.sum(w, axis=1, keepdims=True), 0.0)
            weights.append(w)
        both = jnp.concatenate([vbuf[h, 2 * i], vbuf[h, 2 * i + 1]], axis=1)
        out = jnp.dot(
            jnp.concatenate(weights, axis=0).astype(BF16), both, preferred_element_type=F32
        )
        ohi[i * pair : (i + 1) * pair, :] = jnp.concatenate(
            [out[u * group : (u + 1) * group, u * width : (u + 1) * width] for u in range(2)],
            axis=0,
        ).astype(BF16)

    wide = 2 * rows
    place = lane // wide == -iota((group, 128), 0) % (128 // wide)

    def shifted(x, by):
        return pltpu.roll(x, by % 128, 1) if by % 128 else x

    def statistics(h):
        for off in range(n):
            stat = jnp.where(lane < rows, shifted(tops[h], -off * rows), 0.0)
            total = shifted(sums[h], (1 - off) * rows)
            stat = jnp.where((lane >= rows) & (lane < wide), total, stat)
            by = wide
            while by < 128:
                stat = stat + shifted(stat, by)
                by *= 2
            stat = jnp.sum(jnp.where(place, stat, 0.0), axis=0, keepdims=True)
            if off == 0:
                srecv[h, 0] = stat
            else:
                ssend[h, off] = stat
                remote(
                    ssend.at[h, off], srecv.at[h, off], sss, srs.at[h], source(off)
                ).start()

    def finish(h):
        statistics(h)
        osend[h] = jnp.dot(m[...], ohi[...], preferred_element_type=F32).astype(BF16)
        for off in range(1, n):
            ocopies[h, off] = remote(
                osend.at[h, pl.ds(off * block, block)], orecv.at[h, off],
                oss, ors.at[h], source(off),
            )
            ocopies[h, off].start()

    gather(0)
    for i in range(pairs):
        score(0, i)
    for h in range(kv):
        vcopies[h].wait()
        more = h + 1 < kv
        if more:
            gather(h + 1)
        for i in range(pairs + ahead):
            if more and i >= ahead:
                score(h + 1, i - ahead)
            if i < pairs:
                weigh(h, i)
            if i == pairs - 1:
                finish(h)

    for h in range(kv):
        landed(srecv.at[h, pl.ds(1, n - 1)], srs.at[h])
        stats = [
            pltpu.roll(
                jnp.broadcast_to(srecv[h, off], (group, 128)),
                0, 1, stride=wide, stride_axis=0,
            )
            for off in range(n)
        ]
        best = functools.reduce(jnp.maximum, stats)
        factors = [jnp.exp2(x - best) for x in stats]
        whole = functools.reduce(
            jnp.add, [f * pltpu.roll(x, 128 - rows, 1) for f, x in zip(factors, stats)]
        )
        factors = [f / whole for f in factors]
        landed(orecv.at[h, pl.ds(1, n - 1)], ors.at[h])
        gathered = []
        for off in range(n):
            got = orecv[h, off] if off else osend[h, 0:block, :]
            gathered.append(got.astype(F32).reshape(rows, group, width))
        for r in range(rows):
            total = factors[0][:, r : r + 1] * gathered[0][r]
            for off in range(1, n):
                total = total + factors[off][:, r : r + 1] * gathered[off][r]
            out_ref[r, h * group : (h + 1) * group, :] = total.astype(BF16)

    sent(trecv.at[pl.ds(1, n - 1)], tss)
    sent(qall.at[:, pl.ds(block, (n - 1) * block)], qss)
    sent(osend.at[:, pl.ds(block, (n - 1) * block)], oss)
    sent(srecv.at[:, pl.ds(1, n - 1)], sss)


def on_device(n, queries, page_owner, page_slot, lengths, keys, values):
    pool, kv, tokens, width = keys.shape
    rows, heads, _ = queries.shape
    group = heads // kv
    block = rows * group
    pg = pool * group
    lanes = -(-pool // 128) * 128
    dma = pltpu.SemaphoreType.DMA
    vmem = pl.BlockSpec(memory_space=pltpu.VMEM)
    return pl.pallas_call(
        functools.partial(kernel, n),
        out_shape=pltpu.VMEM(queries.shape, BF16),
        in_specs=[pl.BlockSpec(memory_space=pl.ANY)] * 6,
        out_specs=vmem,
        scratch_shapes=[
            pltpu.SMEM(lengths.shape, jnp.int32),
            pltpu.VMEM(queries.shape, BF16),
            pltpu.VMEM(page_owner.shape, jnp.int32),
            pltpu.VMEM(page_slot.shape, jnp.int32),
            pltpu.VMEM((kv, pool, tokens, width), BF16),
            pltpu.VMEM((kv, pool, tokens, width), BF16),
            pltpu.VMEM((kv, n * block, width), BF16),
            pltpu.VMEM((n, 1, lanes), F32),
            pltpu.VMEM((n, 1, lanes), F32),
            pltpu.VMEM((pg, 128), F32),
            pltpu.VMEM((pg, 128), F32),
            pltpu.VMEM((pg, n * block), BF16),
            pltpu.VMEM((n * block, pg), BF16),
            pltpu.VMEM((2, pg, width), BF16),
            pltpu.VMEM((2, pg, tokens), F32),
            pltpu.VMEM((pg, width), BF16),
            pltpu.VMEM((kv, n * block, width), BF16),
            pltpu.VMEM((kv, n, block, width), BF16),
            pltpu.VMEM((kv, n, 1, 128), F32),
            pltpu.VMEM((kv, n, 1, 128), F32),
            dma((4,)), dma((kv,)), dma((kv,)),
            dma, dma,
            dma, dma((kv,)),
            dma, dma((kv,)),
            dma, dma((kv,)),
        ],
        compiler_params=pltpu.CompilerParams(
            collective_id=0, has_side_effects=True,
            vmem_limit_bytes=66977792
        ),
        name="paged",
    )(lengths, queries, page_owner, page_slot, keys, values)


def solution(mesh):
    placed = (
        P(("groups", "seq", "rep"), "head", None),
        P(("groups", "seq", "rep"), None),
        P(("groups", "seq", "rep"), None),
        P(("groups", "seq", "rep")),
        P(("groups", "seq", "rep"), "head", None, None),
        P(("groups", "seq", "rep"), "head", None, None),
    )
    return jax.shard_map(
        functools.partial(on_device, mesh.shape["seq"]),
        mesh=mesh,
        in_specs=placed,
        out_specs=P(("groups", "seq", "rep"), "head", None),
        check_vma=False,
    )
```

```python
import functools
import math

import jax
import jax.numpy as jnp
from jax import lax
from jax.experimental import pallas as pl
from jax.experimental.pallas import tpu as pltpu
from jax.sharding import PartitionSpec as P

MASKED = -1e30
CODE = 256.0
LATE = 1
DEPTH = 3
F32 = jnp.float32
BF16 = jnp.bfloat16
NT = (((1,), (1,)), ((), ()))


def iota(shape, dim):
    return lax.broadcasted_iota(jnp.int32, shape, dim)


def kernel(
    n, lens_hbm, q_hbm, owner_hbm, slot_hbm, k_hbm, v_hbm, out_ref,
    lens_ref, q_ref, owner_ref, slot_ref, kbuf, vbuf, qall, tsend, trecv, liveb, reqb, mt, m, qslot, wbuf, ohi,
    osend, orecv, ssend, srecv,
    isem, ksem, vsem, tss, trs, qss, qrs, oss, ors, sss, srs,
):
    pool, kv, tokens, width = k_hbm.shape
    rows = q_hbm.shape[0]
    group = q_hbm.shape[1] // kv
    block = rows * group
    lanes = trecv.shape[2]
    scale = math.log2(math.e) / math.sqrt(width)
    me = lax.axis_index("seq")

    def peer(off):
        return {"seq": lax.rem(me + off, n)}

    def source(off):
        return {"seq": lax.rem(me + n - off, n)}

    def remote(src, dst, ssem, rsem, to):
        return pltpu.make_async_remote_copy(
            src_ref=src, dst_ref=dst, send_sem=ssem, recv_sem=rsem,
            device_id=to, device_id_type=pl.DeviceIdType.MESH,
        )

    def landed(ref, sem):
        remote(ref, ref, sem, sem, peer(1)).wait_recv()

    def sent(ref, sem):
        remote(ref, ref, sem, sem, peer(1)).wait_send()

    barrier = pltpu.get_barrier_semaphore()
    for off in range(1, n):
        pl.semaphore_signal(
            barrier, inc=1, device_id=peer(off), device_id_type=pl.DeviceIdType.MESH
        )
    icopies = [
        pltpu.make_async_copy(src, dst, isem.at[i])
        for i, (src, dst) in enumerate((
            (lens_hbm, lens_ref), (owner_hbm, owner_ref), (slot_hbm, slot_ref), (q_hbm, q_ref),
        ))
    ]
    for copy in icopies:
        copy.start()
    kcopies = [pltpu.make_async_copy(k_hbm.at[:, h], kbuf.at[h], ksem.at[h]) for h in range(kv)]
    vcopies = [pltpu.make_async_copy(v_hbm.at[:, h], vbuf.at[h], vsem.at[h]) for h in range(kv)]

    for copy in icopies:
        copy.wait()
    loads = kcopies + vcopies
    for copy in loads[:DEPTH]:
        copy.start()
    span = owner_ref.shape[1]
    row = iota((rows, span), 0)
    length = jnp.zeros((rows, span), jnp.int32)
    for r in range(rows):
        length = jnp.where(row == r, lens_ref[r], length)
    live = jnp.clip(length - iota((rows, span), 1) * tokens, 0, tokens)
    live_f = live.astype(F32)
    owner = owner_ref[...]
    slot = slot_ref[...]
    ones = jnp.ones((8, span), BF16)
    slot_id = iota((pool, span), 0)
    for off in range(n):
        there = lax.rem(me + off, n)
        key = jnp.where((owner == there) & (live > 0), slot, -1)
        acc_live = jnp.zeros((pool, span), F32)
        acc_req = jnp.zeros((pool, span), F32)
        for r in range(rows):
            hit = slot_id == key[r : r + 1, :]
            acc_live = jnp.where(hit, live_f[r : r + 1, :], acc_live)
            acc_req = jnp.where(hit, float(r + 1), acc_req)
        t_live = lax.dot_general(ones, acc_live.astype(BF16), NT, preferred_element_type=F32)
        t_req = lax.dot_general(ones, acc_req.astype(BF16), NT, preferred_element_type=F32)
        table = (t_req * CODE + t_live)[0:1, :]
        if lanes > pool:
            table = jnp.concatenate([table, jnp.zeros((1, lanes - pool), F32)], axis=1)
        if off == 0:
            trecv[0] = table
        else:
            tsend[off] = table

    queries = q_ref[...].astype(F32).reshape(rows, kv, group, width)
    for h in range(kv):
        qall[h, 0:block, :] = queries[:, h].reshape(block, width).astype(BF16)

    pl.semaphore_wait(barrier, n - 1)
    tcopies = {}
    qcopies = {}
    for off in range(1, n):
        tcopies[off] = remote(
            tsend.at[off], trecv.at[off], tss, trs, peer(off)
        )
        tcopies[off].start()
    for h in range(kv):
        for off in range(1, n):
            qcopies[h, off] = remote(
                qall.at[h, pl.ds(0, block)],
                qall.at[h, pl.ds(off * block, block)],
                qss, qrs.at[h], peer(off),
            )

    low = 2 * me < n

    def far_first(copies, down):
        @pl.when(down)
        def _():
            for copy in copies[::-1]:
                copy.start()

        @pl.when(jnp.logical_not(down))
        def _():
            for copy in copies:
                copy.start()

    def send(first, last):
        for h in range(first, last):
            for off in range(1, n):
                qcopies[h, off].start()

    early = lax.axis_index("rep") == 0

    @pl.when(early)
    def _():
        send(0, kv)

    step = math.gcd(pool, 16)
    for h in range(kv):
        kcopies[h].wait()
        for copy in loads[DEPTH + h :] if h == kv - 1 else loads[DEPTH + h : DEPTH + h + 1]:
            copy.start()

        def turn(i, carry):
            for u in range(step):
                kbuf[h, i * step + u] = kbuf[h, i * step + u].T
            return carry

        lax.fori_loop(0, pool // step, turn, 0)
        if h == 0:

            @pl.when(jnp.logical_not(early))
            def _():
                send(0, 1)

        if h == 2:

            @pl.when(jnp.logical_not(early))
            def _():
                send(1, kv)


    landed(trecv.at[pl.ds(1, n - 1)], trs)
    live_row = jnp.zeros((1, lanes), F32)
    req_row = jnp.zeros((1, lanes), F32)
    for off in range(n):
        t = trecv[off]
        request = jnp.floor(t * (1.0 / CODE))
        live_row = live_row + (t - request * CODE)
        req_row = req_row + jnp.where(request > 0.0, request + float(off * rows), 0.0)
    pg = pool * group
    spread = jnp.where(iota((pg, lanes), 0) // group == iota((pg, lanes), 1), 1.0, 0.0)
    spread = spread.astype(BF16)
    liveb[...] = lax.dot_general(
        spread, jnp.broadcast_to(live_row, (128, lanes)).astype(BF16), NT,
        preferred_element_type=F32,
    )
    reqb[...] = lax.dot_general(
        spread, jnp.broadcast_to(req_row, (128, lanes)).astype(BF16), NT,
        preferred_element_type=F32,
    )
    same = iota((pg, 128), 0) % group == iota((pg, 128), 1) % group
    for c in range(n * block // 128):
        want = ((iota((pg, 128), 1) + c * 128) // group + 1).astype(F32)
        mt[:, c * 128 : (c + 1) * 128] = jnp.where(
            same & (reqb[...] == want), 1.0, 0.0
        ).astype(BF16)
    spread_t = jnp.where(iota((lanes, pg), 0) == iota((lanes, pg), 1) // group, 1.0, 0.0)
    req_wide = jnp.dot(
        jnp.broadcast_to(req_row, (8, lanes)).astype(BF16), spread_t.astype(BF16),
        preferred_element_type=F32,
    )[0:1, :]
    same_t = iota((block, pg), 0) % group == iota((block, pg), 1) % group
    for off in range(n):
        want = (iota((block, pg), 0) // group + (off * rows + 1)).astype(F32)
        m[off * block : (off + 1) * block, :] = jnp.where(
            same_t & (req_wide == want), 1.0, 0.0
        ).astype(BF16)

    lane_f = iota((group, 128), 1).astype(F32)
    lane = iota((group, 128), 1)
    pair = 2 * group
    pairs = pool // 2
    ahead = min(8, pairs)
    tops = [jnp.full((group, 128), MASKED, F32) for _ in range(kv)]
    sums = [jnp.zeros((group, 128), F32) for _ in range(kv)]
    ocopies = {}

    def gather(h):
        landed(qall.at[h, pl.ds(block, (n - 1) * block)], qrs.at[h])
        half = pool * group // 2
        for u in range(2):
            at = slice(u * half, (u + 1) * half)
            qslot[h % 2, at, :] = jnp.dot(
                mt[at, :], qall[h], preferred_element_type=F32
            ).astype(BF16)

    def score(h, i):
        keys = jnp.concatenate([kbuf[h, 2 * i], kbuf[h, 2 * i + 1]], axis=1)
        s = jnp.dot(
            qslot[h % 2, i * pair : (i + 1) * pair, :], keys, preferred_element_type=F32
        )
        for u in range(2):
            at = slice((2 * i + u) * group, (2 * i + u + 1) * group)
            x = s[u * group : (u + 1) * group, u * tokens : (u + 1) * tokens]
            x = jnp.where(lane_f < liveb[at, :], x * scale, MASKED)
            wbuf[h % 2, at, :] = x
            pm = jnp.max(x, axis=1, keepdims=True)
            tops[h] = jnp.maximum(
                tops[h], jnp.where(reqb[at, :] == lane_f + 1.0, pm, MASKED)
            )

    def weigh(h, i):
        weights = []
        for u in range(2):
            at = slice((2 * i + u) * group, (2 * i + u + 1) * group)
            mine = reqb[at, :] == lane_f + 1.0
            rm = jnp.max(jnp.where(mine, tops[h], MASKED), axis=1, keepdims=True)
            w = jnp.exp2(wbuf[h % 2, at, :] - rm)
            sums[h] = sums[h] + jnp.where(mine, jnp.sum(w, axis=1, keepdims=True), 0.0)
            weights.append(w)
        both = jnp.concatenate([vbuf[h, 2 * i], vbuf[h, 2 * i + 1]], axis=1)
        out = jnp.dot(
            jnp.concatenate(weights, axis=0).astype(BF16), both, preferred_element_type=F32
        )
        ohi[i * pair : (i + 1) * pair, :] = jnp.concatenate(
            [out[u * group : (u + 1) * group, u * width : (u + 1) * width] for u in range(2)],
            axis=0,
        ).astype(BF16)

    wide = 2 * rows
    place = lane // wide == -iota((group, 128), 0) % (128 // wide)

    def shifted(x, by):
        return pltpu.roll(x, by % 128, 1) if by % 128 else x

    def statistics(h):
        for off in range(n):
            stat = jnp.where(lane < rows, shifted(tops[h], -off * rows), 0.0)
            total = shifted(sums[h], (1 - off) * rows)
            stat = jnp.where((lane >= rows) & (lane < wide), total, stat)
            by = wide
            while by < 128:
                stat = stat + shifted(stat, by)
                by *= 2
            stat = jnp.sum(jnp.where(place, stat, 0.0), axis=0, keepdims=True)
            if off == 0:
                srecv[h, 0] = stat
            else:
                ssend[h, off] = stat
                remote(
                    ssend.at[h, off], srecv.at[h, off], sss, srs.at[h], source(off)
                ).start()

    def finish(h):
        statistics(h)
        osend[h] = jnp.dot(m[...], ohi[...], preferred_element_type=F32).astype(BF16)
        for off in range(1, n):
            ocopies[h, off] = remote(
                osend.at[h, pl.ds(off * block, block)], orecv.at[h, off],
                oss, ors.at[h], source(off),
            )
        far_first([ocopies[h, off] for off in range(1, n)], jnp.logical_not(low))

    gather(0)
    for i in range(pairs):
        score(0, i)
    for h in range(kv):
        vcopies[h].wait()
        more = h + 1 < kv
        if more:
            gather(h + 1)
        for i in range(pairs + ahead):
            if more and i >= ahead:
                score(h + 1, i - ahead)
            if i < pairs:
                weigh(h, i)
            if i == pairs - 1:
                finish(h)

    for h in range(kv):
        landed(srecv.at[h, pl.ds(1, n - 1)], srs.at[h])
        stats = [
            pltpu.roll(
                jnp.broadcast_to(srecv[h, off], (group, 128)),
                0, 1, stride=wide, stride_axis=0,
            )
            for off in range(n)
        ]
        best = functools.reduce(jnp.maximum, stats)
        factors = [jnp.exp2(x - best) for x in stats]
        whole = functools.reduce(
            jnp.add, [f * pltpu.roll(x, 128 - rows, 1) for f, x in zip(factors, stats)]
        )
        factors = [f / whole for f in factors]
        landed(orecv.at[h, pl.ds(1, n - 1)], ors.at[h])
        gathered = []
        for off in range(n):
            got = orecv[h, off] if off else osend[h, 0:block, :]
            gathered.append(got.astype(F32).reshape(rows, group, width))
        for r in range(rows):
            total = factors[0][:, r : r + 1] * gathered[0][r]
            for off in range(1, n):
                total = total + factors[off][:, r : r + 1] * gathered[off][r]
            out_ref[r, h * group : (h + 1) * group, :] = total.astype(BF16)

    sent(trecv.at[pl.ds(1, n - 1)], tss)
    sent(qall.at[:, pl.ds(block, (n - 1) * block)], qss)
    sent(osend.at[:, pl.ds(block, (n - 1) * block)], oss)
    sent(srecv.at[:, pl.ds(1, n - 1)], sss)


def on_device(n, queries, page_owner, page_slot, lengths, keys, values):
    pool, kv, tokens, width = keys.shape
    rows, heads, _ = queries.shape
    group = heads // kv
    block = rows * group
    pg = pool * group
    lanes = -(-pool // 128) * 128
    dma = pltpu.SemaphoreType.DMA
    vmem = pl.BlockSpec(memory_space=pltpu.VMEM)
    return pl.pallas_call(
        functools.partial(kernel, n),
        out_shape=pltpu.VMEM(queries.shape, BF16),
        in_specs=[pl.BlockSpec(memory_space=pl.ANY)] * 6,
        out_specs=vmem,
        scratch_shapes=[
            pltpu.SMEM(lengths.shape, jnp.int32),
            pltpu.VMEM(queries.shape, BF16),
            pltpu.VMEM(page_owner.shape, jnp.int32),
            pltpu.VMEM(page_slot.shape, jnp.int32),
            pltpu.VMEM((kv, pool, tokens, width), BF16),
            pltpu.VMEM((kv, pool, tokens, width), BF16),
            pltpu.VMEM((kv, n * block, width), BF16),
            pltpu.VMEM((n, 1, lanes), F32),
            pltpu.VMEM((n, 1, lanes), F32),
            pltpu.VMEM((pg, 128), F32),
            pltpu.VMEM((pg, 128), F32),
            pltpu.VMEM((pg, n * block), BF16),
            pltpu.VMEM((n * block, pg), BF16),
            pltpu.VMEM((2, pg, width), BF16),
            pltpu.VMEM((2, pg, tokens), F32),
            pltpu.VMEM((pg, width), BF16),
            pltpu.VMEM((kv, n * block, width), BF16),
            pltpu.VMEM((kv, n, block, width), BF16),
            pltpu.VMEM((kv, n, 1, 128), F32),
            pltpu.VMEM((kv, n, 1, 128), F32),
            dma((4,)), dma((kv,)), dma((kv,)),
            dma, dma,
            dma, dma((kv,)),
            dma, dma((kv,)),
            dma, dma((kv,)),
        ],
        compiler_params=pltpu.CompilerParams(
            collective_id=0, has_side_effects=True,
            vmem_limit_bytes=66977792
        ),
        name="paged",
    )(lengths, queries, page_owner, page_slot, keys, values)


def solution(mesh):
    placed = (
        P(("groups", "seq", "rep"), "head", None),
        P(("groups", "seq", "rep"), None),
        P(("groups", "seq", "rep"), None),
        P(("groups", "seq", "rep")),
        P(("groups", "seq", "rep"), "head", None, None),
        P(("groups", "seq", "rep"), "head", None, None),
    )
    return jax.shard_map(
        functools.partial(on_device, mesh.shape["seq"]),
        mesh=mesh,
        in_specs=placed,
        out_specs=P(("groups", "seq", "rep"), "head", None),
        check_vma=False,
    )
```
